32 devices in a mesh: section: 4 (over y, x), seq: 8 (over z, core).
Axes of the slice: x: 2, y: 2, z: 4, core: 2. Of those that a mesh axis runs over, the one named last changes fastest.
Arguments:
- stream: bfloat16 [4, 128, 1536], P('section', 'seq'), may hold values from -6 to 6
- queries: bfloat16 [4, 128, 1536], P('section', 'seq'), may hold values from -40 to 40
- fresh_keys: bfloat16 [4, 128, 1536], P('section', 'seq'), may hold values from -4 to 4
- fresh_values: bfloat16 [4, 128, 1536], P('section', 'seq'), may hold values from -6 to 6
- stale_keys: bfloat16 [4, 1536, 1536], P('section', 'seq'), may hold values from -6 to 6
- stale_values: bfloat16 [4, 1536, 1536], P('section', 'seq'), may hold values from -6 to 6
- gate: float32 [4, 1536], P('section'), may hold values from 0.5 to 4
- patch_of_section: int32 [4], P('section'), may hold values from 0 to 7, as said below
- text_len: int32 [1], replicated, may hold values from 128 to 512
Outputs:
- attended: bfloat16 [4, 128, 1536], P('section', 'seq')
- stream_next: bfloat16 [4, 128, 1536], P('section', 'seq')
The draws below stay inside these ranges and needn't reach their ends.
Inputs may be any that keep to these rules, and one draw needn't show every extreme that they name: `patch_of_section`: section s works on patch (c - s) mod 8 for one c of the draw. The first text_len text positions are used.
All inputs are finite; a program needn't handle non-finite values.
Results may differ from the reference program's by a relative error of at most 0.0085.
Values may be sent and summed in bfloat16 or wider, within the bound.
A program may use at most 64 MiB of HBM per device.

```python
import math
import jax
import jax.numpy as jnp
from jax import lax

HEADS = 12
HDIM = 128
TXT = 512
PATCHES = 8
HW = 1536
PATCH = 128
SEQLEN = 1536
SECTIONS = 4


def joint_draw(key):
    base_key = jax.random.fold_in(key, 7)
    query_seed, key_seed, sign_seed = jax.random.split(base_key, 3)
    full_shape = (SECTIONS, PATCH, HW)
    query_draw = 1.5 * jax.random.truncated_normal(query_seed, -4.0, 4.0, full_shape, jnp.float32)
    key_draw = jax.random.truncated_normal(key_seed, -4.0, 4.0, full_shape, jnp.float32)
    return (query_draw, key_draw)


def draw_queries(key, part):
    return joint_draw(key)[0].astype(jnp.bfloat16)


def draw_fresh_keys(key, part):
    return joint_draw(key)[1].astype(jnp.bfloat16)


def draw_patch_of_section(key, part):
    offset = jax.random.randint(jax.random.fold_in(key, 11), (), 0, PATCHES)
    return ((offset - jnp.arange(SECTIONS, dtype=jnp.int32)) % PATCHES).astype(jnp.int32)


def block_scale(own_key, shape, cuts, low, largest):
    gain = 1.0
    for dim, shards_of in cuts:
        heights = jax.random.uniform(jax.random.fold_in(jax.random.fold_in(own_key, 6), dim), (shards_of,), jnp.float32, low / len(cuts), largest / len(cuts))
        gain = gain * jnp.repeat(jnp.exp(heights), shape[dim] // shards_of).reshape((-1,) + (1,) * (len(shape) - 1 - dim))
    return gain


def scatter_about(key, extent, width, reach, shards=(), kind=jnp.bfloat16):
    loudness = block_scale(key, extent, shards, -0.22, 0.18) if shards else 1.0
    drawn = jax.random.normal(key, extent, jnp.float32) * width * loudness
    return jnp.minimum(jnp.maximum(drawn, -reach), reach).astype(kind)


def setup_inputs(seed: int = 0) -> dict:
    streams_of = jax.random.split(jax.random.key(seed), 10)
    stream = scatter_about(streams_of[0], (SECTIONS, PATCH, HW), 1.0, 6.0, ((0, 4), (1, 8)))
    queries = draw_queries(jax.random.fold_in(streams_of[9], 71), 0)
    fresh_keys = draw_fresh_keys(jax.random.fold_in(streams_of[9], 71), 0)
    fresh_values = scatter_about(streams_of[3], (SECTIONS, PATCH, HW), 1.0, 6.0, ((0, 4), (1, 8)))
    stale_keys = scatter_about(streams_of[4], (SECTIONS, SEQLEN, HW), 1.0, 6.0, ((0, 4), (1, 8)))
    stale_values = scatter_about(streams_of[5], (SECTIONS, SEQLEN, HW), 1.0, 6.0, ((0, 4), (1, 8)))
    gate = jnp.clip(0.5 + 3.5 * jax.random.uniform(streams_of[6], (SECTIONS, HW), jnp.float32) ** block_scale(streams_of[6], (SECTIONS, HW), ((0, 4),), -0.2, 0.2), 0.5, 4.0)
    patch_of_section = draw_patch_of_section(jax.random.fold_in(streams_of[9], 71), 0)
    text_len = jax.random.randint(streams_of[8], (1,), TXT // 4, TXT + 1).astype(jnp.int32)
    return dict(stream=stream, queries=queries, fresh_keys=fresh_keys, fresh_values=fresh_values, stale_keys=stale_keys, stale_values=stale_values, gate=gate, patch_of_section=patch_of_section, text_len=text_len)


def reference(stream, queries, fresh_keys, fresh_values, stale_keys, stale_values, gate, patch_of_section, text_len):
    positions = jnp.arange(SEQLEN, dtype=jnp.int32)
    attended_list = []
    stream_list = []
    for section_index in range(SECTIONS):
        patch_index = patch_of_section[section_index]
        region = (positions - TXT) // PATCH
        stale_ok = jnp.where(positions < TXT, positions < text_len[0], region != patch_index)
        allowed = jnp.concatenate([stale_ok, jnp.ones((PATCH,), dtype=bool)], 0)
        key_block = jnp.concatenate([stale_keys[section_index], fresh_keys[section_index]], 0).astype(jnp.float32).reshape(-1, HEADS, HDIM)
        value_block = jnp.concatenate([stale_values[section_index], fresh_values[section_index]], 0).astype(jnp.float32).reshape(-1, HEADS, HDIM)
        query_block = queries[section_index].astype(jnp.float32).reshape(PATCH, HEADS, HDIM)
        scores = jnp.einsum('qhd,khd->hqk', query_block, key_block) / math.sqrt(HDIM)
        scores = jnp.where(allowed[None, None, :], scores, jnp.float32(-1e+30))
        row_max = lax.optimization_barrier(jnp.max(scores, axis=2))
        weights = jnp.where(allowed[None, None, :], jnp.exp(scores - row_max[:, :, None]), jnp.float32(0.0))
        denominator = lax.optimization_barrier(jnp.sum(weights, axis=2))
        rounded = lax.optimization_barrier(weights.astype(jnp.bfloat16))
        numerator = jnp.einsum('hqk,khd->qhd', rounded.astype(jnp.float32), value_block)
        averaged = numerator / jnp.transpose(denominator)[:, :, None]
        attended_now = averaged.reshape(PATCH, HEADS * HDIM).astype(jnp.bfloat16)
        widened = lax.optimization_barrier(attended_now).astype(jnp.float32)
        incoming = stream[(section_index - 1) % SECTIONS].astype(jnp.float32)
        stream_now = (incoming + gate[section_index][None, :] * widened).astype(jnp.bfloat16)
        attended_list.append(attended_now)
        stream_list.append(stream_now)
    return (jnp.stack(attended_list, 0), jnp.stack(stream_list, 0))
```

```python
import functools
import math

import jax
import jax.numpy as jnp
from jax import lax
from jax.experimental import pallas as pl
from jax.experimental.pallas import tpu as pltpu
from jax.sharding import PartitionSpec as P

HEADS = 12
HDIM = 128
TXT = 512
CORES = 2
HALF = HEADS // CORES
TILES = HALF + 1
LANES = 128
STATS = 8
FLOOR_SCORE = -1e30
SCALE = math.log2(math.e) / math.sqrt(HDIM)
MESH = pl.DeviceIdType.MESH


def query_groups(chips):
    return [list(range(chips))]


def kernel(
    sections,
    chips,
    stream,
    queries,
    fresh_keys,
    fresh_values,
    stale_keys,
    stale_values,
    gate,
    patch_of_section,
    text_len,
    attended_ref,
    stream_ref,
    own_queries,
    all_queries,
    key_rows,
    value_rows,
    part,
    got,
    incoming,
    gate_row,
    patch_scalar,
    text_scalar,
    local_sem,
    query_send,
    query_recv,
    cache_send,
    cache_recv,
    part_send,
    part_recv,
    stream_sem,
):
    me = lax.axis_index("seq")
    section = lax.axis_index("section")
    core = lax.rem(me, CORES)
    chip = me // CORES
    other = 1 - core
    partner = chip * CORES + other
    rows = queries.shape[1]
    stale = stale_keys.shape[1]
    width = HALF * HDIM
    patch_length = rows * chips * CORES

    def columns(which):
        return pl.ds(pl.multiple_of(which * width, width), width)

    def row_slice(start, size):
        return pl.ds(pl.multiple_of(start, 16), size)

    def device(offset, which):
        return lax.rem(chip + offset, chips) * CORES + which

    locals_ = [
        pltpu.make_async_copy(queries.at[0], own_queries, local_sem.at[0]),
        pltpu.make_async_copy(
            queries.at[0, :, columns(core)],
            all_queries.at[row_slice(core * rows, rows)],
            local_sem.at[1],
        ),
        pltpu.make_async_copy(gate, gate_row, local_sem.at[2]),
        pltpu.make_async_copy(patch_of_section, patch_scalar, local_sem.at[3]),
        pltpu.make_async_copy(text_len, text_scalar, local_sem.at[4]),
        pltpu.make_async_copy(
            stale_keys.at[0, :, columns(core)], key_rows.at[pl.ds(0, stale)], local_sem.at[5]
        ),
        pltpu.make_async_copy(
            fresh_keys.at[0, :, columns(core)], key_rows.at[pl.ds(stale, rows)], local_sem.at[6]
        ),
        pltpu.make_async_copy(
            stale_values.at[0, :, columns(core)], value_rows.at[pl.ds(0, stale)], local_sem.at[7]
        ),
        pltpu.make_async_copy(
            fresh_values.at[0, :, columns(core)], value_rows.at[pl.ds(stale, rows)], local_sem.at[8]
        ),
    ]
    for copy in locals_:
        copy.start()

    barrier = pltpu.get_barrier_semaphore()
    for offset in range(chips):
        for which in range(CORES):
            if offset == 0:
                continue
            pl.semaphore_signal(
                barrier, inc=1, device_id={"seq": device(offset, which)}, device_id_type=MESH
            )
    pl.semaphore_signal(barrier, inc=1, device_id={"seq": partner}, device_id_type=MESH)
    pl.semaphore_signal(
        barrier,
        inc=1,
        device_id={"section": lax.rem(section + sections - 1, sections)},
        device_id_type=MESH,
    )
    locals_[0].wait()
    pl.semaphore_wait(barrier, chips * CORES)

    query_copies = []
    for offset in list(range(1, chips)) + [0]:
        back = (chips - offset) % chips
        for which in range(CORES) if offset else (other,):
            target = device(offset, which)
            query_copies.append(
                pltpu.make_async_remote_copy(
                    src_ref=own_queries.at[:, columns(which)],
                    dst_ref=all_queries.at[row_slice(back * CORES * rows + core * rows, rows)],
                    send_sem=query_send.at[offset, which],
                    recv_sem=query_recv.at[back, core],
                    device_id={"seq": target},
                    device_id_type=MESH,
                )
            )
            query_copies[-1].start()

    base = stale + rows
    cache_copies = []
    for number, (source, start, size, target) in enumerate(
        (
            (stale_keys, base, stale, key_rows),
            (fresh_keys, base + stale, rows, key_rows),
            (stale_values, base, stale, value_rows),
            (fresh_values, base + stale, rows, value_rows),
        )
    ):
        cache_copies.append(
            pltpu.make_async_remote_copy(
                src_ref=source.at[0, :, columns(other)],
                dst_ref=target.at[pl.ds(start, size)],
                send_sem=cache_send.at[number],
                recv_sem=cache_recv.at[number],
                device_id={"seq": partner},
                device_id_type=MESH,
            )
        )
        cache_copies[-1].start()

    stream_copy = pltpu.make_async_remote_copy(
        src_ref=stream.at[0],
        dst_ref=incoming,
        send_sem=stream_sem.at[0],
        recv_sem=stream_sem.at[1],
        device_id={"section": lax.rem(section + 1, sections)},
        device_id_type=MESH,
    )
    stream_copy.start()

    for copy in locals_[1:]:
        copy.wait()

    total = CORES * base
    column = lax.broadcasted_iota(jnp.int32, (1, total), 1)
    second = column >= base
    inner = jnp.where(second, column - base, column)
    owner = jnp.where(second, partner, me)
    position = owner * stale + inner
    first_banned = TXT + patch_scalar[0] * patch_length
    banned = (position >= first_banned) & (position < first_banned + patch_length)
    unused_text = (position < TXT) & (position >= text_scalar[0])
    banned = (banned & (position >= TXT)) | unused_text
    allowed = (inner >= stale) | jnp.logical_not(banned)
    penalty = jnp.where(allowed, 0.0, FLOOR_SCORE)

    for number in range(4):
        cache_copies[number].wait_recv()

    part_copies = []
    own_copy = None
    for group in query_groups(chips):
        for offset in group:
            for which in range(CORES) if offset else (other,):
                pltpu.make_async_remote_copy(
                    src_ref=own_queries.at[:, columns(which)],
                    dst_ref=all_queries.at[row_slice(offset * CORES * rows + which * rows, rows)],
                    send_sem=query_send.at[offset, which],
                    recv_sem=query_recv.at[offset, which],
                    device_id={"seq": device(offset, which)},
                    device_id_type=MESH,
                ).wait_recv()
        low = group[0] * CORES * rows
        count = len(group) * CORES * rows
        span = pl.ds(low, count)
        lane = lax.broadcasted_iota(jnp.int32, (count, LANES), 1)
        lane_head = lax.rem(lane, STATS)
        spread = jnp.zeros((count, LANES), jnp.float32)
        for head in range(HALF):
            wide = pl.ds(head * HDIM, HDIM)
            scores = lax.dot_general(
                all_queries[span, wide],
                key_rows[:, wide],
                (((1,), (1,)), ((), ())),
                preferred_element_type=jnp.float32,
            )
            scores = scores * SCALE + penalty
            largest = jnp.max(scores, axis=1, keepdims=True)
            weights = jnp.exp2(scores - largest)
            amount = jnp.sum(weights, axis=1, keepdims=True)
            summed = jnp.dot(
                weights.astype(jnp.bfloat16),
                value_rows[:, wide],
                preferred_element_type=jnp.float32,
            )
            part[head, span] = (summed / amount).astype(jnp.bfloat16)
            spread = jnp.where(lane_head == head, largest + jnp.log2(amount), spread)
        high = spread.astype(jnp.bfloat16).astype(jnp.float32)
        rest = spread - high
        middle = rest.astype(jnp.bfloat16).astype(jnp.float32)
        low_term = rest - middle
        part[HALF, span] = jnp.where(
            lane < STATS, high, jnp.where(lane < 2 * STATS, middle, low_term)
        ).astype(jnp.bfloat16)
        for offset in group:
            back = (chips - offset) % chips
            for which in range(CORES) if offset else (other,):
                copy = pltpu.make_async_remote_copy(
                    src_ref=part.at[:, row_slice(offset * CORES * rows + which * rows, rows)],
                    dst_ref=got.at[back, core],
                    send_sem=part_send.at[offset, which],
                    recv_sem=part_recv.at[back, core],
                    device_id={"seq": device(offset, which)},
                    device_id_type=MESH,
                )
                copy.start()
                part_copies.append(copy)
            if offset == 0:
                own_copy = pltpu.make_async_copy(
                    part.at[:, row_slice(core * rows, rows)], got.at[0, core], local_sem.at[9]
                )
                own_copy.start()

    own_copy.wait()
    stream_copy.wait_recv()
    for offset in range(chips):
        for which in range(CORES) if offset else (other,):
            pltpu.make_async_remote_copy(
                src_ref=part.at[:, row_slice(which * rows, rows)],
                dst_ref=got.at[offset, which],
                send_sem=part_send.at[offset, which],
                recv_sem=part_recv.at[offset, which],
                device_id={"seq": device(offset, which)},
                device_id_type=MESH,
            ).wait_recv()

    for which in range(CORES):
        logs = []
        for offset in range(chips):
            terms = got[offset, which, HALF].astype(jnp.float32)
            logs.append(
                terms
                + pltpu.roll(terms, LANES - STATS, 1)
                + pltpu.roll(terms, LANES - 2 * STATS, 1)
            )
        largest = functools.reduce(jnp.maximum, logs)
        shares = [jnp.exp2(log - largest) for log in logs]
        whole = functools.reduce(jnp.add, shares)
        shares = [share / whole for share in shares]
        for head in range(HALF):
            wide = pl.ds((which * HALF + head) * HDIM, HDIM)
            mean = functools.reduce(
                jnp.add,
                [
                    shares[offset][:, head : head + 1]
                    * got[offset, which, head].astype(jnp.float32)
                    for offset in range(chips)
                ],
            )
            rounded = mean.astype(jnp.bfloat16)
            attended_ref[0, :, wide] = rounded
            stream_ref[0, :, wide] = (
                incoming[:, wide].astype(jnp.float32)
                + gate_row[:, wide] * rounded.astype(jnp.float32)
            ).astype(jnp.bfloat16)

    for copy in query_copies + cache_copies + [stream_copy] + part_copies:
        copy.wait_send()


def local(*arguments):
    sections = lax.axis_size("section")
    count = lax.axis_size("seq")
    chips = count // CORES
    queries, stale_keys = arguments[1], arguments[4]
    rows, channels = queries.shape[1:]
    cached = CORES * (stale_keys.shape[1] + rows)
    width = HALF * HDIM
    everyone = rows * count
    anywhere = pl.BlockSpec(memory_space=pl.ANY)
    inside = pl.BlockSpec(memory_space=pltpu.VMEM)
    result = jax.ShapeDtypeStruct((1, rows, channels), jnp.bfloat16)
    return pl.pallas_call(
        functools.partial(kernel, sections, chips),
        out_shape=(result, result),
        in_specs=[anywhere] * 9,
        out_specs=(inside, inside),
        scratch_shapes=[
            pltpu.VMEM((rows, channels), jnp.bfloat16),
            pltpu.VMEM((everyone, width), jnp.bfloat16),
            pltpu.VMEM((cached, width), jnp.bfloat16),
            pltpu.VMEM((cached, width), jnp.bfloat16),
            pltpu.VMEM((TILES, everyone, HDIM), jnp.bfloat16),
            pltpu.VMEM((chips, CORES, TILES, rows, HDIM), jnp.bfloat16),
            pltpu.VMEM((rows, channels), jnp.bfloat16),
            pltpu.VMEM((1, channels), jnp.float32),
            pltpu.SMEM((1,), jnp.int32),
            pltpu.SMEM((1,), jnp.int32),
            pltpu.SemaphoreType.DMA((10,)),
            pltpu.SemaphoreType.DMA((chips, CORES)),
            pltpu.SemaphoreType.DMA((chips, CORES)),
            pltpu.SemaphoreType.DMA((4,)),
            pltpu.SemaphoreType.DMA((4,)),
            pltpu.SemaphoreType.DMA((chips, CORES)),
            pltpu.SemaphoreType.DMA((chips, CORES)),
            pltpu.SemaphoreType.DMA((2,)),
        ],
        compiler_params=pltpu.CompilerParams(collective_id=0, has_side_effects=True),
    )(*arguments)


def solution(mesh):
    placed = (
        P("section", "seq", None),
        P("section", "seq", None),
        P("section", "seq", None),
        P("section", "seq", None),
        P("section", "seq", None),
        P("section", "seq", None),
        P("section", None),
        P("section"),
        P(),
    )
    return jax.shard_map(
        local,
        mesh=mesh,
        in_specs=placed,
        out_specs=(P("section", "seq", None), P("section", "seq", None)),
        check_vma=False,
    )
```

```python
import functools
import math

import jax
import jax.numpy as jnp
from jax import lax
from jax.experimental import pallas as pl
from jax.experimental.pallas import tpu as pltpu
from jax.sharding import PartitionSpec as P

HEADS = 12
HDIM = 128
TXT = 512
CORES = 2
HALF = HEADS // CORES
TILES = HALF + 1
LANES = 128
STATS = 8
FLOOR_SCORE = -1e30
SCALE = math.log2(math.e) / math.sqrt(HDIM)
MESH = pl.DeviceIdType.MESH


def query_groups(chips):
    return [[0], list(range(1, chips))]


def kernel(
    sections,
    chips,
    stream,
    queries,
    fresh_keys,
    fresh_values,
    stale_keys,
    stale_values,
    gate,
    patch_of_section,
    text_len,
    results,
    own_queries,
    all_queries,
    key_rows,
    value_rows,
    part,
    got,
    incoming,
    gate_row,
    patch_scalar,
    text_scalar,
    local_sem,
    query_send,
    query_recv,
    cache_send,
    cache_recv,
    part_send,
    part_recv,
    stream_sem,
):
    me = lax.axis_index("seq")
    section = lax.axis_index("section")
    core = lax.rem(me, CORES)
    chip = me // CORES
    other = 1 - core
    partner = chip * CORES + other
    rows = queries.shape[1]
    stale = stale_keys.shape[1]
    width = HALF * HDIM
    patch_length = rows * chips * CORES

    def columns(which):
        return pl.ds(pl.multiple_of(which * width, width), width)

    def row_slice(start, size):
        return pl.ds(pl.multiple_of(start, 16), size)

    def device(offset, which):
        return lax.rem(chip + offset, chips) * CORES + which

    locals_ = [
        pltpu.make_async_copy(queries.at[0], own_queries, local_sem.at[0]),
        pltpu.make_async_copy(
            queries.at[0, :, columns(core)],
            all_queries.at[row_slice(core * rows, rows)],
            local_sem.at[1],
        ),
        pltpu.make_async_copy(gate, gate_row, local_sem.at[2]),
        pltpu.make_async_copy(patch_of_section, patch_scalar, local_sem.at[3]),
        pltpu.make_async_copy(text_len, text_scalar, local_sem.at[4]),
        pltpu.make_async_copy(
            stale_keys.at[0, :, columns(core)], key_rows.at[pl.ds(0, stale)], local_sem.at[5]
        ),
        pltpu.make_async_copy(
            fresh_keys.at[0, :, columns(core)], key_rows.at[pl.ds(stale, rows)], local_sem.at[6]
        ),
        pltpu.make_async_copy(
            stale_values.at[0, :, columns(core)], value_rows.at[pl.ds(0, stale)], local_sem.at[7]
        ),
        pltpu.make_async_copy(
            fresh_values.at[0, :, columns(core)], value_rows.at[pl.ds(stale, rows)], local_sem.at[8]
        ),
    ]
    for copy in locals_:
        copy.start()

    barrier = pltpu.get_barrier_semaphore()
    for offset in range(chips):
        for which in range(CORES):
            if offset == 0:
                continue
            pl.semaphore_signal(
                barrier, inc=1, device_id={"seq": device(offset, which)}, device_id_type=MESH
            )
    pl.semaphore_signal(barrier, inc=1, device_id={"seq": partner}, device_id_type=MESH)
    pl.semaphore_signal(
        barrier,
        inc=1,
        device_id={"section": lax.rem(section + sections - 1, sections)},
        device_id_type=MESH,
    )
    locals_[0].wait()
    pl.semaphore_wait(barrier, chips * CORES)

    query_copies = []
    for offset in list(range(1, chips)) + [0]:
        back = (chips - offset) % chips
        for which in range(CORES) if offset else (other,):
            target = device(offset, which)
            query_copies.append(
                pltpu.make_async_remote_copy(
                    src_ref=own_queries.at[:, columns(which)],
                    dst_ref=all_queries.at[row_slice(back * CORES * rows + core * rows, rows)],
                    send_sem=query_send.at[offset, which],
                    recv_sem=query_recv.at[back, core],
                    device_id={"seq": target},
                    device_id_type=MESH,
                )
            )
            query_copies[-1].start()

    base = stale + rows
    cache_copies = []
    for number, (source, start, size, target) in enumerate(
        (
            (stale_keys, base, stale, key_rows),
            (fresh_keys, base + stale, rows, key_rows),
            (stale_values, base, stale, value_rows),
            (fresh_values, base + stale, rows, value_rows),
        )
    ):
        cache_copies.append(
            pltpu.make_async_remote_copy(
                src_ref=source.at[0, :, columns(other)],
                dst_ref=target.at[pl.ds(start, size)],
                send_sem=cache_send.at[number],
                recv_sem=cache_recv.at[number],
                device_id={"seq": partner},
                device_id_type=MESH,
            )
        )
        cache_copies[-1].start()

    stream_copy = pltpu.make_async_remote_copy(
        src_ref=stream.at[0],
        dst_ref=incoming,
        send_sem=stream_sem.at[0],
        recv_sem=stream_sem.at[1],
        device_id={"section": lax.rem(section + 1, sections)},
        device_id_type=MESH,
    )
    stream_copy.start()

    for copy in locals_[1:]:
        copy.wait()

    total = CORES * base
    column = lax.broadcasted_iota(jnp.int32, (1, total), 1)
    second = column >= base
    inner = jnp.where(second, column - base, column)
    owner = jnp.where(second, partner, me)
    position = owner * stale + inner
    first_banned = TXT + patch_scalar[0] * patch_length
    banned = (position >= first_banned) & (position < first_banned + patch_length)
    unused_text = (position < TXT) & (position >= text_scalar[0])
    banned = (banned & (position >= TXT)) | unused_text
    allowed = (inner >= stale) | jnp.logical_not(banned)
    penalty = jnp.where(allowed, 0.0, FLOOR_SCORE)

    for number in range(4):
        cache_copies[number].wait_recv()

    part_copies = []
    own_copy = None
    for group in query_groups(chips):
        for offset in group:
            for which in range(CORES) if offset else (other,):
                pltpu.make_async_remote_copy(
                    src_ref=own_queries.at[:, columns(which)],
                    dst_ref=all_queries.at[row_slice(offset * CORES * rows + which * rows, rows)],
                    send_sem=query_send.at[offset, which],
                    recv_sem=query_recv.at[offset, which],
                    device_id={"seq": device(offset, which)},
                    device_id_type=MESH,
                ).wait_recv()
        low = group[0] * CORES * rows
        count = len(group) * CORES * rows
        span = pl.ds(low, count)
        lane = lax.broadcasted_iota(jnp.int32, (count, LANES), 1)
        lane_head = lax.rem(lane, STATS)
        spread = jnp.zeros((count, LANES), jnp.float32)
        for head in range(HALF):
            wide = pl.ds(head * HDIM, HDIM)
            scores = lax.dot_general(
                all_queries[span, wide],
                key_rows[:, wide],
                (((1,), (1,)), ((), ())),
                preferred_element_type=jnp.float32,
            )
            scores = scores * SCALE + penalty
            largest = jnp.max(scores, axis=1, keepdims=True)
            weights = jnp.exp2(scores - largest)
            amount = jnp.sum(weights, axis=1, keepdims=True)
            summed = jnp.dot(
                weights.astype(jnp.bfloat16),
                value_rows[:, wide],
                preferred_element_type=jnp.float32,
            )
            part[head, span] = (summed / amount).astype(jnp.bfloat16)
            spread = jnp.where(lane_head == head, largest + jnp.log2(amount), spread)
        high = spread.astype(jnp.bfloat16).astype(jnp.float32)
        rest = spread - high
        middle = rest.astype(jnp.bfloat16).astype(jnp.float32)
        low_term = rest - middle
        part[HALF, span] = jnp.where(
            lane < STATS, high, jnp.where(lane < 2 * STATS, middle, low_term)
        ).astype(jnp.bfloat16)
        for offset in group:
            back = (chips - offset) % chips
            for which in range(CORES) if offset else (other,):
                copy = pltpu.make_async_remote_copy(
                    src_ref=part.at[:, row_slice(offset * CORES * rows + which * rows, rows)],
                    dst_ref=got.at[back, core],
                    send_sem=part_send.at[offset, which],
                    recv_sem=part_recv.at[back, core],
                    device_id={"seq": device(offset, which)},
                    device_id_type=MESH,
                )
                copy.start()
                part_copies.append(copy)
            if offset == 0:
                own_copy = pltpu.make_async_copy(
                    part.at[:, row_slice(core * rows, rows)], got.at[0, core], local_sem.at[9]
                )
                own_copy.start()

    own_copy.wait()
    stream_copy.wait_recv()
    for offset in range(chips):
        for which in range(CORES) if offset else (other,):
            pltpu.make_async_remote_copy(
                src_ref=part.at[:, row_slice(which * rows, rows)],
                dst_ref=got.at[offset, which],
                send_sem=part_send.at[offset, which],
                recv_sem=part_recv.at[offset, which],
                device_id={"seq": device(offset, which)},
                device_id_type=MESH,
            ).wait_recv()

    for which in range(CORES):
        logs = []
        for offset in range(chips):
            terms = got[offset, which, HALF].astype(jnp.float32)
            logs.append(
                terms
                + pltpu.roll(terms, LANES - STATS, 1)
                + pltpu.roll(terms, LANES - 2 * STATS, 1)
            )
        largest = functools.reduce(jnp.maximum, logs)
        shares = [jnp.exp2(log - largest) for log in logs]
        whole = functools.reduce(jnp.add, shares)
        shares = [share / whole for share in shares]
        for head in range(HALF):
            wide = pl.ds((which * HALF + head) * HDIM, HDIM)
            mean = functools.reduce(
                jnp.add,
                [
                    shares[offset][:, head : head + 1]
                    * got[offset, which, head].astype(jnp.float32)
                    for offset in range(chips)
                ],
            )
            rounded = mean.astype(jnp.bfloat16)
            results[0, 0, :, wide] = rounded
            results[1, 0, :, wide] = (
                incoming[:, wide].astype(jnp.float32)
                + gate_row[:, wide] * rounded.astype(jnp.float32)
            ).astype(jnp.bfloat16)

    for copy in query_copies + cache_copies + [stream_copy] + part_copies:
        copy.wait_send()


def local(*arguments):
    sections = lax.axis_size("section")
    count = lax.axis_size("seq")
    chips = count // CORES
    queries, stale_keys = arguments[1], arguments[4]
    rows, channels = queries.shape[1:]
    cached = CORES * (stale_keys.shape[1] + rows)
    width = HALF * HDIM
    everyone = rows * count
    anywhere = pl.BlockSpec(memory_space=pl.ANY)
    inside = pl.BlockSpec(memory_space=pltpu.VMEM)
    result = pltpu.VMEM((2, 1, rows, channels), jnp.bfloat16)
    results = pl.pallas_call(
        functools.partial(kernel, sections, chips),
        out_shape=result,
        in_specs=[anywhere] * 9,
        out_specs=inside,
        scratch_shapes=[
            pltpu.VMEM((rows, channels), jnp.bfloat16),
            pltpu.VMEM((everyone, width), jnp.bfloat16),
            pltpu.VMEM((cached, width), jnp.bfloat16),
            pltpu.VMEM((cached, width), jnp.bfloat16),
            pltpu.VMEM((TILES, everyone, HDIM), jnp.bfloat16),
            pltpu.VMEM((chips, CORES, TILES, rows, HDIM), jnp.bfloat16),
            pltpu.VMEM((rows, channels), jnp.bfloat16),
            pltpu.VMEM((1, channels), jnp.float32),
            pltpu.SMEM((1,), jnp.int32),
            pltpu.SMEM((1,), jnp.int32),
            pltpu.SemaphoreType.DMA((10,)),
            pltpu.SemaphoreType.DMA((chips, CORES)),
            pltpu.SemaphoreType.DMA((chips, CORES)),
            pltpu.SemaphoreType.DMA((4,)),
            pltpu.SemaphoreType.DMA((4,)),
            pltpu.SemaphoreType.DMA((chips, CORES)),
            pltpu.SemaphoreType.DMA((chips, CORES)),
            pltpu.SemaphoreType.DMA((2,)),
        ],
        compiler_params=pltpu.CompilerParams(collective_id=0, has_side_effects=True),
    )(*arguments)
    return (results[0], results[1])


def solution(mesh):
    placed = (
        P("section", "seq", None),
        P("section", "seq", None),
        P("section", "seq", None),
        P("section", "seq", None),
        P("section", "seq", None),
        P("section", "seq", None),
        P("section", None),
        P("section"),
        P(),
    )
    return jax.shard_map(
        local,
        mesh=mesh,
        in_specs=placed,
        out_specs=(P("section", "seq", None), P("section", "seq", None)),
        check_vma=False,
    )
```

```python
import functools
import math

import jax
import jax.numpy as jnp
from jax import lax
from jax.experimental import pallas as pl
from jax.experimental.pallas import tpu as pltpu
from jax.sharding import PartitionSpec as P

HEADS = 12
HDIM = 128
TXT = 512
CORES = 2
HALF = HEADS // CORES
TILES = HALF + 1
LANES = 128
STATS = 8
FLOOR_SCORE = -1e30
SCALE = math.log2(math.e) / math.sqrt(HDIM)
MESH = pl.DeviceIdType.MESH


def query_groups(chips):
    return [[0], list(range(1, chips))]


def kernel(
    sections,
    chips,
    stream,
    queries,
    fresh_keys,
    fresh_values,
    stale_keys,
    stale_values,
    gate,
    patch_of_section,
    text_len,
    results,
    own_queries,
    all_queries,
    key_rows,
    value_rows,
    part,
    got,
    incoming,
    gate_row,
    patch_scalar,
    text_scalar,
    local_sem,
    query_send,
    query_recv,
    cache_send,
    cache_recv,
    part_send,
    part_recv,
    stream_sem,
):
    me = lax.axis_index("seq")
    section = lax.axis_index("section")
    core = lax.rem(me, CORES)
    chip = me // CORES
    other = 1 - core
    partner = chip * CORES + other
    rows = queries.shape[1]
    stale = stale_keys.shape[1]
    width = HALF * HDIM
    patch_length = rows * chips * CORES

    def columns(which):
        return pl.ds(pl.multiple_of(which * width, width), width)

    def row_slice(start, size):
        return pl.ds(pl.multiple_of(start, 16), size)

    def device(offset, which):
        return lax.rem(chip + offset, chips) * CORES + which

    barrier = pltpu.get_barrier_semaphore()
    for offset in range(chips):
        for which in range(CORES):
            if offset == 0:
                continue
            pl.semaphore_signal(
                barrier, inc=1, device_id={"seq": device(offset, which)}, device_id_type=MESH
            )
    pl.semaphore_signal(barrier, inc=1, device_id={"seq": partner}, device_id_type=MESH)
    pl.semaphore_signal(
        barrier,
        inc=1,
        device_id={"section": lax.rem(section + sections - 1, sections)},
        device_id_type=MESH,
    )
    locals_ = [
        pltpu.make_async_copy(queries.at[0], own_queries, local_sem.at[0]),
        pltpu.make_async_copy(
            queries.at[0, :, columns(core)],
            all_queries.at[row_slice(core * rows, rows)],
            local_sem.at[1],
        ),
        pltpu.make_async_copy(gate, gate_row, local_sem.at[2]),
        pltpu.make_async_copy(patch_of_section, patch_scalar, local_sem.at[3]),
        pltpu.make_async_copy(text_len, text_scalar, local_sem.at[4]),
        pltpu.make_async_copy(
            stale_keys.at[0, :, columns(core)], key_rows.at[pl.ds(0, stale)], local_sem.at[5]
        ),
        pltpu.make_async_copy(
            fresh_keys.at[0, :, columns(core)], key_rows.at[pl.ds(stale, rows)], local_sem.at[6]
        ),
        pltpu.make_async_copy(
            stale_values.at[0, :, columns(core)], value_rows.at[pl.ds(0, stale)], local_sem.at[7]
        ),
        pltpu.make_async_copy(
            fresh_values.at[0, :, columns(core)], value_rows.at[pl.ds(stale, rows)], local_sem.at[8]
        ),
    ]
    for copy in locals_:
        copy.start()

    locals_[0].wait()
    pl.semaphore_wait(barrier, chips * CORES)

    query_copies = []
    for offset in list(range(1, chips)) + [0]:
        back = (chips - offset) % chips
        for which in range(CORES) if offset else (other,):
            target = device(offset, which)
            query_copies.append(
                pltpu.make_async_remote_copy(
                    src_ref=own_queries.at[:, columns(which)],
                    dst_ref=all_queries.at[row_slice(back * CORES * rows + core * rows, rows)],
                    send_sem=query_send.at[offset, which],
                    recv_sem=query_recv.at[back, core],
                    device_id={"seq": target},
                    device_id_type=MESH,
                )
            )
            query_copies[-1].start()

    base = stale + rows
    cache_copies = []
    for number, (source, start, size, target) in enumerate(
        (
            (stale_keys, base, stale, key_rows),
            (fresh_keys, base + stale, rows, key_rows),
            (stale_values, base, stale, value_rows),
            (fresh_values, base + stale, rows, value_rows),
        )
    ):
        cache_copies.append(
            pltpu.make_async_remote_copy(
                src_ref=source.at[0, :, columns(other)],
                dst_ref=target.at[pl.ds(start, size)],
                send_sem=cache_send.at[number],
                recv_sem=cache_recv.at[number],
                device_id={"seq": partner},
                device_id_type=MESH,
            )
        )
        cache_copies[-1].start()

    stream_copy = pltpu.make_async_remote_copy(
        src_ref=stream.at[0],
        dst_ref=incoming,
        send_sem=stream_sem.at[0],
        recv_sem=stream_sem.at[1],
        device_id={"section": lax.rem(section + 1, sections)},
        device_id_type=MESH,
    )
    stream_copy.start()

    for copy in locals_[1:]:
        copy.wait()

    total = CORES * base
    column = lax.broadcasted_iota(jnp.int32, (1, total), 1)
    second = column >= base
    inner = jnp.where(second, column - base, column)
    owner = jnp.where(second, partner, me)
    position = owner * stale + inner
    first_banned = TXT + patch_scalar[0] * patch_length
    banned = (position >= first_banned) & (position < first_banned + patch_length)
    unused_text = (position < TXT) & (position >= text_scalar[0])
    banned = (banned & (position >= TXT)) | unused_text
    allowed = (inner >= stale) | jnp.logical_not(banned)
    penalty = jnp.where(allowed, 0.0, FLOOR_SCORE)

    for number in range(4):
        cache_copies[number].wait_recv()

    part_copies = []
    own_copy = None
    for group in query_groups(chips):
        for offset in group:
            for which in range(CORES) if offset else (other,):
                pltpu.make_async_remote_copy(
                    src_ref=own_queries.at[:, columns(which)],
                    dst_ref=all_queries.at[row_slice(offset * CORES * rows + which * rows, rows)],
                    send_sem=query_send.at[offset, which],
                    recv_sem=query_recv.at[offset, which],
                    device_id={"seq": device(offset, which)},
                    device_id_type=MESH,
                ).wait_recv()
        low = group[0] * CORES * rows
        count = len(group) * CORES * rows
        span = pl.ds(low, count)
        lane = lax.broadcasted_iota(jnp.int32, (count, LANES), 1)
        lane_head = lax.rem(lane, STATS)
        spread = jnp.zeros((count, LANES), jnp.float32)
        for head in range(HALF):
            wide = pl.ds(head * HDIM, HDIM)
            scores = lax.dot_general(
                all_queries[span, wide],
                key_rows[:, wide],
                (((1,), (1,)), ((), ())),
                preferred_element_type=jnp.float32,
            )
            scores = scores * SCALE + penalty
            largest = jnp.max(scores, axis=1, keepdims=True)
            weights = jnp.exp2(scores - largest)
            amount = jnp.sum(weights, axis=1, keepdims=True)
            summed = jnp.dot(
                weights.astype(jnp.bfloat16),
                value_rows[:, wide],
                preferred_element_type=jnp.float32,
            )
            part[head, span] = (summed / amount).astype(jnp.bfloat16)
            spread = jnp.where(lane_head == head, largest + jnp.log2(amount), spread)
        high = spread.astype(jnp.bfloat16).astype(jnp.float32)
        rest = spread - high
        middle = rest.astype(jnp.bfloat16).astype(jnp.float32)
        low_term = rest - middle
        part[HALF, span] = jnp.where(
            lane < STATS, high, jnp.where(lane < 2 * STATS, middle, low_term)
        ).astype(jnp.bfloat16)
        for offset in group:
            back = (chips - offset) % chips
            for which in range(CORES) if offset else (other,):
                copy = pltpu.make_async_remote_copy(
                    src_ref=part.at[:, row_slice(offset * CORES * rows + which * rows, rows)],
                    dst_ref=got.at[back, core],
                    send_sem=part_send.at[offset, which],
                    recv_sem=part_recv.at[back, core],
                    device_id={"seq": device(offset, which)},
                    device_id_type=MESH,
                )
                copy.start()
                part_copies.append(copy)
            if offset == 0:
                own_copy = pltpu.make_async_copy(
                    part.at[:, row_slice(core * rows, rows)], got.at[0, core], local_sem.at[9]
                )
                own_copy.start()

    own_copy.wait()
    stream_copy.wait_recv()
    for offset in range(chips):
        for which in range(CORES) if offset else (other,):
            pltpu.make_async_remote_copy(
                src_ref=part.at[:, row_slice(which * rows, rows)],
                dst_ref=got.at[offset, which],
                send_sem=part_send.at[offset, which],
                recv_sem=part_recv.at[offset, which],
                device_id={"seq": device(offset, which)},
                device_id_type=MESH,
            ).wait_recv()

    for which in range(CORES):
        logs = []
        for offset in range(chips):
            terms = got[offset, which, HALF].astype(jnp.float32)
            logs.append(
                terms
                + pltpu.roll(terms, LANES - STATS, 1)
                + pltpu.roll(terms, LANES - 2 * STATS, 1)
            )
        largest = functools.reduce(jnp.maximum, logs)
        shares = [jnp.exp2(log - largest) for log in logs]
        whole = functools.reduce(jnp.add, shares)
        shares = [share / whole for share in shares]
        for head in range(HALF):
            wide = pl.ds((which * HALF + head) * HDIM, HDIM)
            mean = functools.reduce(
                jnp.add,
                [
                    shares[offset][:, head : head + 1]
                    * got[offset, which, head].astype(jnp.float32)
                    for offset in range(chips)
                ],
            )
            rounded = mean.astype(jnp.bfloat16)
            results[0, 0, :, wide] = rounded
            results[1, 0, :, wide] = (
                incoming[:, wide].astype(jnp.float32)
                + gate_row[:, wide] * rounded.astype(jnp.float32)
            ).astype(jnp.bfloat16)

    for copy in query_copies + cache_copies + [stream_copy] + part_copies:
        copy.wait_send()


def local(*arguments):
    sections = lax.axis_size("section")
    count = lax.axis_size("seq")
    chips = count // CORES
    queries, stale_keys = arguments[1], arguments[4]
    rows, channels = queries.shape[1:]
    cached = CORES * (stale_keys.shape[1] + rows)
    width = HALF * HDIM
    everyone = rows * count
    anywhere = pl.BlockSpec(memory_space=pl.ANY)
    inside = pl.BlockSpec(memory_space=pltpu.VMEM)
    result = pltpu.VMEM((2, 1, rows, channels), jnp.bfloat16)
    results = pl.pallas_call(
        functools.partial(kernel, sections, chips),
        out_shape=result,
        in_specs=[anywhere] * 9,
        out_specs=inside,
        scratch_shapes=[
            pltpu.VMEM((rows, channels), jnp.bfloat16),
            pltpu.VMEM((everyone, width), jnp.bfloat16),
            pltpu.VMEM((cached, width), jnp.bfloat16),
            pltpu.VMEM((cached, width), jnp.bfloat16),
            pltpu.VMEM((TILES, everyone, HDIM), jnp.bfloat16),
            pltpu.VMEM((chips, CORES, TILES, rows, HDIM), jnp.bfloat16),
            pltpu.VMEM((rows, channels), jnp.bfloat16),
            pltpu.VMEM((1, channels), jnp.float32),
            pltpu.SMEM((1,), jnp.int32),
            pltpu.SMEM((1,), jnp.int32),
            pltpu.SemaphoreType.DMA((10,)),
            pltpu.SemaphoreType.DMA((chips, CORES)),
            pltpu.SemaphoreType.DMA((chips, CORES)),
            pltpu.SemaphoreType.DMA((4,)),
            pltpu.SemaphoreType.DMA((4,)),
            pltpu.SemaphoreType.DMA((chips, CORES)),
            pltpu.SemaphoreType.DMA((chips, CORES)),
            pltpu.SemaphoreType.DMA((2,)),
        ],
        compiler_params=pltpu.CompilerParams(collective_id=0, has_side_effects=True),
    )(*arguments)
    return (results[0], results[1])


def solution(mesh):
    placed = (
        P("section", "seq", None),
        P("section", "seq", None),
        P("section", "seq", None),
        P("section", "seq", None),
        P("section", "seq", None),
        P("section", "seq", None),
        P("section", None),
        P("section"),
        P(),
    )
    return jax.shard_map(
        local,
        mesh=mesh,
        in_specs=placed,
        out_specs=(P("section", "seq", None), P("section", "seq", None)),
        check_vma=False,
    )
```
